32 devices in a mesh: src: 4 (over y, x), rcv: 8 (over z, core).
Axes of the slice: x: 2, y: 2, z: 4, core: 2. Of those that a mesh axis runs over, the one named last changes fastest.
Arguments:
- wavefield: float32 [2, 16, 2048, 2048], P(None, None, 'rcv', 'src')
- surface_band: float32 [2, 2048, 1024], P(None, 'rcv'), may hold values from -0.75 to 0.75
- band_shift: int32 [32], P('rcv'), may hold values from -16 to 16
- trace_mask: int32 [2048], P('rcv'), may hold values 0 or 1
- shot_taper: float32 [5], replicated, may hold values from 0.2 to 1
Outputs:
- multiples: float32 [2, 16, 2048, 2048], P(None, None, 'rcv', 'src')
- primaries: float32 [2, 16, 2048, 2048], P(None, None, 'rcv', 'src')
The draws below stay inside these ranges and needn't reach their ends.
All inputs are finite; a program needn't handle non-finite values. No bound on the sum of `trace_mask` on one device may be relied on, other than what follows from the above.
Results may differ from the reference program's by a relative error of at most 0.0003.
Values sent between devices are 32-bit elements; how exact they have to be, the bound alone decides.
A program may use at most 192 MiB of HBM per device.

```python
import jax
import jax.numpy as jnp
from jax import lax

F = 16
NS = 2048
NR = 2048
APER = 64
SHIFT = 16
BLOCK = 64
SHALF = 2


def draw_wavefield(key, part):
    base_key = jax.random.fold_in(key, 7)
    noise_key, row_key, col_key = jax.random.split(base_key, 3)
    rows = jnp.exp(jax.random.uniform(row_key, (NS,), jnp.float32, -1.15, 1.15)) * jnp.exp(1.0986 * (jnp.arange(NS, dtype=jnp.float32) / NS - 0.5))
    cols = jnp.exp(jax.random.uniform(col_key, (NR,), jnp.float32, -1.15, 1.15)) * jnp.exp(1.0986 * (jnp.arange(NR, dtype=jnp.float32) / NR - 0.5))
    noise = jax.random.normal(noise_key, (2, F, NR, NS), jnp.float32)
    return noise * cols[None, None, :, None] * rows[None, None, None, :] * 0.5


def touch_ends(array, key, least, largest):
    place = [jax.random.randint(jax.random.fold_in(key, axis), (), 0, length) for axis, length in enumerate(array.shape)]
    longest = array.shape.index(max(array.shape))
    neighbour = place[:longest] + [(place[longest] + 1) % array.shape[longest]] + place[longest + 1:]
    return array.at[tuple(place)].set(least).at[tuple(neighbour)].set(largest)


def levels(stream_key, extent, cuts, low, top_value):
    level, own = 1.0, jax.random.fold_in(stream_key, 6)
    for position, shards_of in cuts:
        heights = jnp.exp(jax.random.uniform(jax.random.fold_in(own, position), (shards_of,), jnp.float32, low / len(cuts), top_value / len(cuts)))
        level = level * jnp.repeat(heights, extent[position] // shards_of).reshape([-1 if axis == position else 1 for axis in range(len(extent))])
    return level


def gaussian(stream_key, extent, spread, limit, shards=(), kind=jnp.bfloat16):
    level = levels(stream_key, extent, shards, -0.22, 0.18) if shards else 1.0
    drawn = jax.random.normal(stream_key, extent, jnp.float32) * spread * level
    return jnp.minimum(jnp.maximum(drawn, -limit), limit).astype(kind)


def setup_inputs(seed: int = 0) -> dict:
    key_of = jax.random.split(jax.random.key(seed), 6)
    wavefield = draw_wavefield(jax.random.fold_in(key_of[5], 71), 0)
    surface_band = gaussian(key_of[1], (2, NR, F * APER), APER ** -0.5, 0.75, ((1, 8),), jnp.float32)
    band_shift = touch_ends(jax.random.randint(key_of[2], (NR // BLOCK,), -SHIFT, SHIFT + 1), jax.random.fold_in(key_of[2], 1), -SHIFT, SHIFT).astype(jnp.int32)
    trace_mask = touch_ends((jax.random.randint(key_of[3], (NR,), 0, 8) < 7).astype(jnp.int32), jax.random.fold_in(key_of[3], 1), 0, 1)
    shot_taper = jnp.clip(jax.random.uniform(key_of[4], (2 * SHALF + 1,), jnp.float32, 0.2, 1.0), 0.2, 1.0)
    return dict(wavefield=wavefield, surface_band=surface_band, band_shift=band_shift, trace_mask=trace_mask, shot_taper=shot_taper)


def band_matrix(band_piece):
    columns = band_piece.shape[3]
    taps = band_piece.shape[2]
    rows_index = jnp.arange(columns + taps - 1, dtype=jnp.int32)
    cols_index = jnp.arange(columns, dtype=jnp.int32)
    tap_index = jnp.arange(taps, dtype=jnp.int32)
    onehot = (tap_index[:, None, None] == rows_index[None, :, None] - cols_index[None, None, :]).astype(jnp.float32)
    return jnp.einsum('xftc,tjc->xfjc', band_piece, onehot, precision=lax.Precision.HIGHEST)

def complex_product(window, band):
    real_part = jnp.einsum('fjc,fjs->fcs', band[0], window[0], precision=lax.Precision.HIGHEST) - jnp.einsum('fjc,fjs->fcs', band[1], window[1], precision=lax.Precision.HIGHEST)
    imag_part = jnp.einsum('fjc,fjs->fcs', band[1], window[0], precision=lax.Precision.HIGHEST) + jnp.einsum('fjc,fjs->fcs', band[0], window[1], precision=lax.Precision.HIGHEST)
    return jnp.stack([real_part, imag_part])

def reference(wavefield, surface_band, band_shift, trace_mask, shot_taper):
    masked = wavefield * trace_mask.astype(jnp.float32)[None, None, :, None]
    halo_width = APER // 2 + SHIFT
    padded = jnp.pad(masked, ((0, 0), (0, 0), (halo_width, halo_width), (0, 0)))
    band_full = jnp.transpose(surface_band.reshape(2, NR, F, APER), (0, 2, 3, 1))

    def one_block(index):
        start = index * BLOCK + halo_width - APER // 2 + band_shift[index]
        window = lax.dynamic_slice_in_dim(padded, start.astype(jnp.int32), BLOCK + APER - 1, 2)
        band_piece = lax.dynamic_slice_in_dim(band_full, (index * BLOCK).astype(jnp.int32), BLOCK, 3)
        return complex_product(window, band_matrix(band_piece))
    stacked = lax.map(one_block, jnp.arange(NR // BLOCK, dtype=jnp.int32))
    predicted = jnp.moveaxis(stacked, 0, 2).reshape(2, F, NR, NS)
    shot_padded = jnp.pad(predicted, ((0, 0), (0, 0), (0, 0), (SHALF, SHALF)))
    multiples = jnp.zeros_like(predicted)
    for offset_row in range(2 * SHALF + 1):
        multiples = multiples + shot_taper[offset_row] * shot_padded[:, :, :, offset_row:offset_row + NS]
    data_energy = lax.optimization_barrier(jnp.sum(wavefield * wavefield, axis=(0, 2, 3)))
    pred_energy = lax.optimization_barrier(jnp.sum(multiples * multiples, axis=(0, 2, 3)))
    gain = jnp.sqrt((data_energy + 1e-06) / (pred_energy + 1e-06))
    primaries = wavefield - gain[None, :, None, None] * multiples
    return (multiples, primaries)
```

```python
import functools

import jax
import jax.numpy as jnp
from jax import lax
from jax.experimental import pallas as pl
from jax.experimental.pallas import tpu as pltpu
from jax.sharding import PartitionSpec as P

APER = 64
SHIFT = 16
BLOCK = 64
SHALF = 2
LANES = 128
HALO = APER // 2 + SHIFT
CHUNKS = 4
MESH = pl.DeviceIdType.MESH


def shifted(cells, axis, step):
    count = lax.axis_size(axis)
    ends = count - 1
    if step > 0:
        pairs = [(i, i + 1) for i in range(ends)]
    else:
        pairs = [(i + 1, i) for i in range(ends)]
    return lax.ppermute(cells, axis, pairs)


def split(cells):
    high = cells.astype(jnp.bfloat16)
    low = (cells - high.astype(jnp.float32)).astype(jnp.bfloat16)
    return high, low


def predict_kernel(first, shift_ref, taper_ref, wave_ref, mask_ref, above_ref, below_ref, side_ref, band_ref, *refs):
    mult_ref, energy_ref, rows_ref = refs[-3:]
    step = pl.program_id(0)
    here = first + step
    receivers, shots = wave_ref.shape[2:]
    width = shots + LANES

    data = jnp.float32(0)
    for x in range(2):
        wave = wave_ref[x, 0]
        data = data + jnp.sum(wave * wave)
        rows_ref[x, HALO : HALO + receivers, :shots] = wave * mask_ref[...]
        rows_ref[x, :HALO, :shots] = above_ref[x, 0]
        rows_ref[x, HALO + receivers : receivers + 2 * HALO, :shots] = below_ref[x, 0]
        rows_ref[x, : receivers + 2 * HALO, shots:] = side_ref[x, 0]

    odd = here % 2 == 1
    lane = lax.broadcasted_iota(jnp.int32, (BLOCK, LANES), 1)

    def skewed(x, index):
        taps = band_ref[x, index * BLOCK : (index + 1) * BLOCK, :]
        taps = jnp.where(odd, pltpu.roll(taps, LANES - APER, 1), taps)
        taps = jnp.where(lane < APER, taps, 0.0)
        return pltpu.roll(taps, 0, 1, stride=1, stride_axis=0)

    def near(x, whole, rest):
        tall = rows_ref[x, pl.ds(whole, 2 * BLOCK + 8), :]
        return pltpu.roll(tall, (2 * BLOCK + 8 - rest) % (2 * BLOCK + 8), 0)[: 2 * BLOCK]

    total = jnp.zeros((8, shots), jnp.float32)
    for index in range(receivers // BLOCK):
        start = index * BLOCK + HALO - APER // 2 + shift_ref[index]
        rest = start & 7
        whole = pl.multiple_of(start - rest, 8)
        window = jnp.concatenate([near(x, whole, rest) for x in range(2)], axis=0)
        high, low = split(window)
        real, imag = skewed(0, index), skewed(1, index)
        weights = jnp.concatenate(
            [jnp.concatenate([real, -imag], axis=1), jnp.concatenate([imag, real], axis=1)], axis=0
        )
        weights_high, weights_low = split(weights)
        both = jnp.concatenate([weights_high, weights_low], axis=0)
        upper = jnp.dot(both, high, preferred_element_type=jnp.float32)
        lower = jnp.dot(weights_high, low, preferred_element_type=jnp.float32)
        pred = upper[: 2 * BLOCK] + (upper[2 * BLOCK :] + lower)
        mult = taper_ref[SHALF] * pred[:, :shots]
        for u in range(2 * SHALF + 1):
            if u != SHALF:
                mult = mult + taper_ref[u] * pltpu.roll(pred, (SHALF - u) % width, 1)[:, :shots]
        mult_ref[0, 0, index * BLOCK : (index + 1) * BLOCK, :] = mult[:BLOCK]
        mult_ref[1, 0, index * BLOCK : (index + 1) * BLOCK, :] = mult[BLOCK:]
        total = total + jnp.sum((mult * mult).reshape(-1, 8, shots), axis=0)

    row = lax.broadcasted_iota(jnp.int32, (8, LANES), 0)
    col = lax.broadcasted_iota(jnp.int32, (8, LANES), 1)
    news = jnp.where(row == 0, data, jnp.sum(total))
    news = jnp.where((row < 2) & (col == here), news, 0.0)

    @pl.when(step == 0)
    def _():
        energy_ref[...] = jnp.zeros_like(energy_ref)

    energy_ref[...] += news


def predict(first, count, wave, mask, above, below, side, band, band_shift, shot_taper, mult):
    _, slices, receivers, shots = wave.shape
    in_specs = [
        pl.BlockSpec(memory_space=pltpu.SMEM),
        pl.BlockSpec(memory_space=pltpu.SMEM),
        pl.BlockSpec((2, 1, receivers, shots), lambda g: (0, first + g, 0, 0)),
        pl.BlockSpec((receivers, 1), lambda g: (0, 0)),
        pl.BlockSpec((2, 1, HALO, shots), lambda g: (0, g, 0, 0)),
        pl.BlockSpec((2, 1, HALO, shots), lambda g: (0, g, 0, 0)),
        pl.BlockSpec((2, 1, receivers + 2 * HALO, LANES), lambda g: (0, first + g, 0, 0)),
        pl.BlockSpec((2, receivers, LANES), lambda g: (0, 0, (first + g) // 2)),
    ]
    args = [band_shift, shot_taper, wave, mask, above, below, side, band]
    aliases = {}
    if mult is not None:
        in_specs.append(pl.BlockSpec(memory_space=pl.ANY))
        aliases = {len(args): 0}
        args.append(mult)
    flops = 3 * 2 * 4 * BLOCK * 4 * BLOCK * count * (receivers // BLOCK) * (shots + LANES)
    return pl.pallas_call(
        functools.partial(predict_kernel, first),
        grid=(count,),
        in_specs=in_specs,
        out_specs=[
            pl.BlockSpec((2, 1, receivers, shots), lambda g: (0, first + g, 0, 0)),
            pl.BlockSpec((8, LANES), lambda g: (0, 0)),
        ],
        out_shape=[
            jax.ShapeDtypeStruct(wave.shape, jnp.float32),
            jax.ShapeDtypeStruct((8, LANES), jnp.float32),
        ],
        scratch_shapes=[pltpu.VMEM((2, receivers + 2 * HALO + 8, shots + LANES), jnp.float32)],
        input_output_aliases=aliases,
        cost_estimate=pl.CostEstimate(
            flops=flops, bytes_accessed=count * receivers * shots * 20, transcendentals=0
        ),
        compiler_params=pltpu.CompilerParams(
            dimension_semantics=("arbitrary",), vmem_limit_bytes=48 * 2**20
        ),
        name=f"predict{first}",
    )(*args)


def gain_kernel(axes, *refs):
    energies, (gain_ref, mine, plane, space, local_sem, send_a, recv_a, send_b, recv_b) = refs[:-9], refs[-9:]
    (slow, slow_count), (fast, fast_count) = axes
    slow_me, fast_me = lax.axis_index(slow), lax.axis_index(fast)

    def slow_peer(d):
        return {slow: lax.rem(slow_me + d, slow_count)}

    def fast_peer(d):
        return {fast: lax.rem(fast_me + d, fast_count)}

    barrier = pltpu.get_barrier_semaphore()
    for d in range(1, slow_count):
        pl.semaphore_signal(barrier, inc=1, device_id=slow_peer(d), device_id_type=MESH)
    for d in range(1, fast_count):
        pl.semaphore_signal(barrier, inc=1, device_id=fast_peer(d), device_id_type=MESH)
    total = energies[0][...]
    for other in energies[1:]:
        total = total + other[...]
    mine[...] = total
    own = pltpu.make_async_copy(mine, plane.at[0], local_sem)
    own.start()
    pl.semaphore_wait(barrier, slow_count + fast_count - 2)

    copies = []
    for d in range(1, slow_count):
        copy = pltpu.make_async_remote_copy(
            src_ref=mine, dst_ref=plane.at[d], send_sem=send_a.at[d], recv_sem=recv_a.at[d],
            device_id=slow_peer(d), device_id_type=MESH,
        )
        copy.start()
        copies.append(copy)
    own.wait()
    for copy in copies:
        copy.wait()
    copies = []
    for d in range(1, fast_count):
        copy = pltpu.make_async_remote_copy(
            src_ref=plane, dst_ref=space.at[d - 1], send_sem=send_b.at[d], recv_sem=recv_b.at[d],
            device_id=fast_peer(d), device_id_type=MESH,
        )
        copy.start()
        copies.append(copy)
    total = jnp.sum(plane[...], axis=0)
    for copy in copies:
        copy.wait()
    for d in range(fast_count - 1):
        total = total + jnp.sum(space[d], axis=0)
    data = jnp.broadcast_to(total[0:1], total.shape)
    pred = jnp.broadcast_to(total[1:2], total.shape)
    gain_ref[...] = jnp.sqrt((data + 1e-06) / (pred + 1e-06))


def gains(energies, axes, identity):
    slow_count, fast_count = axes[0][1], axes[1][1]
    return pl.pallas_call(
        functools.partial(gain_kernel, axes),
        in_specs=[pl.BlockSpec(memory_space=pltpu.VMEM)] * len(energies),
        out_specs=pl.BlockSpec(memory_space=pltpu.VMEM),
        out_shape=jax.ShapeDtypeStruct((8, LANES), jnp.float32),
        scratch_shapes=[
            pltpu.VMEM((8, LANES), jnp.float32),
            pltpu.VMEM((slow_count, 8, LANES), jnp.float32),
            pltpu.VMEM((fast_count - 1, slow_count, 8, LANES), jnp.float32),
            pltpu.SemaphoreType.DMA,
            pltpu.SemaphoreType.DMA((slow_count,)),
            pltpu.SemaphoreType.DMA((slow_count,)),
            pltpu.SemaphoreType.DMA((fast_count,)),
            pltpu.SemaphoreType.DMA((fast_count,)),
        ],
        cost_estimate=pl.CostEstimate(flops=1000, bytes_accessed=8 * 2**20, transcendentals=0),
        compiler_params=pltpu.CompilerParams(collective_id=identity, has_side_effects=True),
        name=f"gains{identity}",
    )(*energies)


def subtract_kernel(first, gain_ref, wave_ref, mult_ref, *refs):
    prim_ref = refs[-1]
    here = first + pl.program_id(0)
    col = lax.broadcasted_iota(jnp.int32, (1, LANES), 1)
    gain = jnp.sum(jnp.where(col == here, gain_ref[0:1, :], 0.0))
    prim_ref[...] = wave_ref[...] - gain * mult_ref[...]


def subtract(first, count, gain, wave, mult, prim):
    _, slices, receivers, shots = wave.shape
    block = pl.BlockSpec((2, 1, receivers, shots), lambda g: (0, first + g, 0, 0))
    in_specs = [pl.BlockSpec((8, LANES), lambda g: (0, 0)), block, block]
    args = [gain, wave, mult]
    aliases = {}
    if prim is not None:
        in_specs.append(pl.BlockSpec(memory_space=pl.ANY))
        aliases = {len(args): 0}
        args.append(prim)
    return pl.pallas_call(
        functools.partial(subtract_kernel, first),
        grid=(count,),
        in_specs=in_specs,
        out_specs=block,
        out_shape=jax.ShapeDtypeStruct(wave.shape, jnp.float32),
        input_output_aliases=aliases,
        cost_estimate=pl.CostEstimate(
            flops=0, bytes_accessed=count * receivers * shots * 24, transcendentals=0
        ),
        compiler_params=pltpu.CompilerParams(
            dimension_semantics=("arbitrary",), vmem_limit_bytes=48 * 2**20
        ),
        name=f"subtract{first}",
    )(*args)


def per_device(wavefield, surface_band, band_shift, trace_mask, shot_taper):
    _, slices, receivers, shots = wavefield.shape
    mask = trace_mask.astype(jnp.float32)
    size = slices // CHUNKS

    halos = []
    for c in range(CHUNKS):
        part = wavefield[:, c * size : (c + 1) * size]
        tail = part[:, :, receivers - HALO :] * mask[None, None, receivers - HALO :, None]
        head = part[:, :, :HALO] * mask[None, None, :HALO, None]
        halos.append((shifted(tail, "rcv", 1), shifted(head, "rcv", -1)))

    first = jnp.swapaxes(wavefield[..., :SHALF] * mask[None, None, :, None], 2, 3)
    last = jnp.swapaxes(wavefield[..., shots - SHALF :] * mask[None, None, :, None], 2, 3)
    after = shifted(first, "src", -1)
    before = shifted(last, "src", 1)
    sides = jnp.concatenate([after, before], axis=2)
    sides = jnp.concatenate(
        [
            shifted(sides[..., receivers - HALO :], "rcv", 1),
            sides,
            shifted(sides[..., :HALO], "rcv", -1),
        ],
        axis=3,
    )
    gap = jnp.zeros((2, slices, LANES - 2 * SHALF, receivers + 2 * HALO), jnp.float32)
    side = jnp.swapaxes(jnp.concatenate([sides[:, :, :SHALF], gap, sides[:, :, SHALF:]], axis=2), 2, 3)

    column = mask[:, None]
    mult = None
    energies = []
    for c in range(CHUNKS):
        mult, energy = predict(
            c * size, size, wavefield, column, *halos[c], side, surface_band, band_shift, shot_taper, mult
        )
        energies.append(energy)
    axes = (("src", lax.axis_size("src")), ("rcv", lax.axis_size("rcv")))
    gain = gains(energies, axes, 1)
    prim = subtract(0, slices, gain, wavefield, mult, None)
    return (mult, prim)


def solution(mesh):
    in_specs = (P(None, None, "rcv", "src"), P(None, "rcv", None), P("rcv"), P("rcv"), P())
    out_specs = (P(None, None, "rcv", "src"), P(None, None, "rcv", "src"))
    return jax.shard_map(
        per_device, mesh=mesh, in_specs=in_specs, out_specs=out_specs, check_vma=False
    )
```

```python
import functools

import jax
import jax.numpy as jnp
from jax import lax
from jax.experimental import pallas as pl
from jax.experimental.pallas import tpu as pltpu
from jax.sharding import PartitionSpec as P

APER = 64
SHIFT = 16
BLOCK = 64
SHALF = 2
LANES = 128
HALO = APER // 2 + SHIFT
CHUNKS = 2
MESH = pl.DeviceIdType.MESH


def shifted(cells, axis, step):
    count = lax.axis_size(axis)
    ends = count - 1
    if step > 0:
        pairs = [(i, i + 1) for i in range(ends)]
    else:
        pairs = [(i + 1, i) for i in range(ends)]
    return lax.ppermute(cells, axis, pairs)


def split(cells):
    high = cells.astype(jnp.bfloat16)
    low = (cells - high.astype(jnp.float32)).astype(jnp.bfloat16)
    return high, low


def predict_kernel(first, shift_ref, taper_ref, wave_ref, mask_ref, above_ref, below_ref, side_ref, band_ref, *refs):
    mult_ref, energy_ref, rows_ref = refs[-3:]
    step = pl.program_id(0)
    here = first + step
    receivers, shots = wave_ref.shape[2:]
    width = shots + LANES

    data = jnp.float32(0)
    for x in range(2):
        wave = wave_ref[x, 0]
        data = data + jnp.sum(wave * wave)
        rows_ref[x, HALO : HALO + receivers, :shots] = wave * mask_ref[...]
        rows_ref[x, :HALO, :shots] = above_ref[x, 0]
        rows_ref[x, HALO + receivers : receivers + 2 * HALO, :shots] = below_ref[x, 0]
        rows_ref[x, : receivers + 2 * HALO, shots:] = side_ref[x, 0]

    odd = here % 2 == 1
    lane = lax.broadcasted_iota(jnp.int32, (BLOCK, LANES), 1)

    def skewed(x, index):
        taps = band_ref[x, index * BLOCK : (index + 1) * BLOCK, :]
        taps = jnp.where(odd, pltpu.roll(taps, LANES - APER, 1), taps)
        taps = jnp.where(lane < APER, taps, 0.0)
        return pltpu.roll(taps, 0, 1, stride=1, stride_axis=0)

    def near(x, whole, rest):
        tall = rows_ref[x, pl.ds(whole, 2 * BLOCK + 8), :]
        return pltpu.roll(tall, (2 * BLOCK + 8 - rest) % (2 * BLOCK + 8), 0)[: 2 * BLOCK]

    total = jnp.zeros((8, shots), jnp.float32)
    for index in range(receivers // BLOCK):
        start = index * BLOCK + HALO - APER // 2 + shift_ref[index]
        rest = start & 7
        whole = pl.multiple_of(start - rest, 8)
        window = jnp.concatenate([near(x, whole, rest) for x in range(2)], axis=0)
        high, low = split(window)
        real, imag = skewed(0, index), skewed(1, index)
        weights = jnp.concatenate(
            [jnp.concatenate([real, -imag], axis=1), jnp.concatenate([imag, real], axis=1)], axis=0
        )
        weights_high, weights_low = split(weights)
        both = jnp.concatenate([weights_high, weights_low], axis=0)
        upper = jnp.dot(both, high, preferred_element_type=jnp.float32)
        lower = jnp.dot(weights_high, low, preferred_element_type=jnp.float32)
        pred = upper[: 2 * BLOCK] + (upper[2 * BLOCK :] + lower)
        mult = taper_ref[SHALF] * pred[:, :shots]
        for u in range(2 * SHALF + 1):
            if u != SHALF:
                mult = mult + taper_ref[u] * pltpu.roll(pred, (SHALF - u) % width, 1)[:, :shots]
        mult_ref[0, 0, index * BLOCK : (index + 1) * BLOCK, :] = mult[:BLOCK]
        mult_ref[1, 0, index * BLOCK : (index + 1) * BLOCK, :] = mult[BLOCK:]
        total = total + jnp.sum((mult * mult).reshape(-1, 8, shots), axis=0)

    row = lax.broadcasted_iota(jnp.int32, (8, LANES), 0)
    col = lax.broadcasted_iota(jnp.int32, (8, LANES), 1)
    news = jnp.where(row == 0, data, jnp.sum(total))
    news = jnp.where((row < 2) & (col == here), news, 0.0)

    @pl.when(step == 0)
    def _():
        energy_ref[...] = jnp.zeros_like(energy_ref)

    energy_ref[...] += news


def predict(first, count, wave, mask, above, below, side, band, band_shift, shot_taper, mult):
    _, slices, receivers, shots = wave.shape
    in_specs = [
        pl.BlockSpec(memory_space=pltpu.SMEM),
        pl.BlockSpec(memory_space=pltpu.SMEM),
        pl.BlockSpec((2, 1, receivers, shots), lambda g: (0, first + g, 0, 0)),
        pl.BlockSpec((receivers, 1), lambda g: (0, 0)),
        pl.BlockSpec((2, 1, HALO, shots), lambda g: (0, g, 0, 0)),
        pl.BlockSpec((2, 1, HALO, shots), lambda g: (0, g, 0, 0)),
        pl.BlockSpec((2, 1, receivers + 2 * HALO, LANES), lambda g: (0, first + g, 0, 0)),
        pl.BlockSpec((2, receivers, LANES), lambda g: (0, 0, (first + g) // 2)),
    ]
    args = [band_shift, shot_taper, wave, mask, above, below, side, band]
    aliases = {}
    if mult is not None:
        in_specs.append(pl.BlockSpec(memory_space=pl.ANY))
        aliases = {len(args): 0}
        args.append(mult)
    flops = 3 * 2 * 4 * BLOCK * 4 * BLOCK * count * (receivers // BLOCK) * (shots + LANES)
    return pl.pallas_call(
        functools.partial(predict_kernel, first),
        grid=(count,),
        in_specs=in_specs,
        out_specs=[
            pl.BlockSpec((2, 1, receivers, shots), lambda g: (0, first + g, 0, 0)),
            pl.BlockSpec((8, LANES), lambda g: (0, 0)),
        ],
        out_shape=[
            jax.ShapeDtypeStruct(wave.shape, jnp.float32),
            jax.ShapeDtypeStruct((8, LANES), jnp.float32),
        ],
        scratch_shapes=[pltpu.VMEM((2, receivers + 2 * HALO + 8, shots + LANES), jnp.float32)],
        input_output_aliases=aliases,
        cost_estimate=pl.CostEstimate(
            flops=flops, bytes_accessed=count * receivers * shots * 20, transcendentals=0
        ),
        compiler_params=pltpu.CompilerParams(
            dimension_semantics=("arbitrary",), vmem_limit_bytes=48 * 2**20
        ),
        name=f"predict{first}",
    )(*args)


def gain_kernel(axes, *refs):
    energies, (gain_ref, mine, plane, space, local_sem, send_a, recv_a, send_b, recv_b) = refs[:-9], refs[-9:]
    (slow, slow_count), (fast, fast_count) = axes
    slow_me, fast_me = lax.axis_index(slow), lax.axis_index(fast)

    def slow_peer(d):
        return {slow: lax.rem(slow_me + d, slow_count)}

    def fast_peer(d):
        return {fast: lax.rem(fast_me + d, fast_count)}

    barrier = pltpu.get_barrier_semaphore()
    for d in range(1, slow_count):
        pl.semaphore_signal(barrier, inc=1, device_id=slow_peer(d), device_id_type=MESH)
    for d in range(1, fast_count):
        pl.semaphore_signal(barrier, inc=1, device_id=fast_peer(d), device_id_type=MESH)
    total = energies[0][...]
    for other in energies[1:]:
        total = total + other[...]
    mine[...] = total
    own = pltpu.make_async_copy(mine, plane.at[0], local_sem)
    own.start()
    pl.semaphore_wait(barrier, slow_count + fast_count - 2)

    copies = []
    for d in range(1, slow_count):
        copy = pltpu.make_async_remote_copy(
            src_ref=mine, dst_ref=plane.at[d], send_sem=send_a.at[d], recv_sem=recv_a.at[d],
            device_id=slow_peer(d), device_id_type=MESH,
        )
        copy.start()
        copies.append(copy)
    own.wait()
    for copy in copies:
        copy.wait()
    copies = []
    for d in range(1, fast_count):
        copy = pltpu.make_async_remote_copy(
            src_ref=plane, dst_ref=space.at[d - 1], send_sem=send_b.at[d], recv_sem=recv_b.at[d],
            device_id=fast_peer(d), device_id_type=MESH,
        )
        copy.start()
        copies.append(copy)
    total = jnp.sum(plane[...], axis=0)
    for copy in copies:
        copy.wait()
    for d in range(fast_count - 1):
        total = total + jnp.sum(space[d], axis=0)
    data = jnp.broadcast_to(total[0:1], total.shape)
    pred = jnp.broadcast_to(total[1:2], total.shape)
    gain_ref[...] = jnp.sqrt((data + 1e-06) / (pred + 1e-06))


def gains(energies, axes, identity):
    slow_count, fast_count = axes[0][1], axes[1][1]
    return pl.pallas_call(
        functools.partial(gain_kernel, axes),
        in_specs=[pl.BlockSpec(memory_space=pltpu.VMEM)] * len(energies),
        out_specs=pl.BlockSpec(memory_space=pltpu.VMEM),
        out_shape=jax.ShapeDtypeStruct((8, LANES), jnp.float32),
        scratch_shapes=[
            pltpu.VMEM((8, LANES), jnp.float32),
            pltpu.VMEM((slow_count, 8, LANES), jnp.float32),
            pltpu.VMEM((fast_count - 1, slow_count, 8, LANES), jnp.float32),
            pltpu.SemaphoreType.DMA,
            pltpu.SemaphoreType.DMA((slow_count,)),
            pltpu.SemaphoreType.DMA((slow_count,)),
            pltpu.SemaphoreType.DMA((fast_count,)),
            pltpu.SemaphoreType.DMA((fast_count,)),
        ],
        cost_estimate=pl.CostEstimate(flops=1000, bytes_accessed=8 * 2**20, transcendentals=0),
        compiler_params=pltpu.CompilerParams(collective_id=identity, has_side_effects=True),
        name=f"gains{identity}",
    )(*energies)


def subtract_kernel(first, gain_ref, wave_ref, mult_ref, *refs):
    prim_ref = refs[-1]
    here = first + pl.program_id(0)
    col = lax.broadcasted_iota(jnp.int32, (1, LANES), 1)
    gain = jnp.sum(jnp.where(col == here, gain_ref[0:1, :], 0.0))
    prim_ref[...] = wave_ref[...] - gain * mult_ref[...]


def subtract(first, count, gain, wave, mult, prim):
    _, slices, receivers, shots = wave.shape
    block = pl.BlockSpec((2, 1, receivers, shots), lambda g: (0, first + g, 0, 0))
    in_specs = [pl.BlockSpec((8, LANES), lambda g: (0, 0)), block, block]
    args = [gain, wave, mult]
    aliases = {}
    if prim is not None:
        in_specs.append(pl.BlockSpec(memory_space=pl.ANY))
        aliases = {len(args): 0}
        args.append(prim)
    return pl.pallas_call(
        functools.partial(subtract_kernel, first),
        grid=(count,),
        in_specs=in_specs,
        out_specs=block,
        out_shape=jax.ShapeDtypeStruct(wave.shape, jnp.float32),
        input_output_aliases=aliases,
        cost_estimate=pl.CostEstimate(
            flops=0, bytes_accessed=count * receivers * shots * 24, transcendentals=0
        ),
        compiler_params=pltpu.CompilerParams(
            dimension_semantics=("arbitrary",), vmem_limit_bytes=48 * 2**20
        ),
        name=f"subtract{first}",
    )(*args)


def per_device(wavefield, surface_band, band_shift, trace_mask, shot_taper):
    _, slices, receivers, shots = wavefield.shape
    mask = trace_mask.astype(jnp.float32)
    size = slices // CHUNKS

    halos = []
    for c in range(CHUNKS):
        part = wavefield[:, c * size : (c + 1) * size]
        tail = part[:, :, receivers - HALO :] * mask[None, None, receivers - HALO :, None]
        head = part[:, :, :HALO] * mask[None, None, :HALO, None]
        halos.append((shifted(tail, "rcv", 1), shifted(head, "rcv", -1)))

    pick = jnp.eye(SHALF, LANES, dtype=jnp.float32)
    turn = functools.partial(jnp.einsum, precision=lax.Precision.HIGHEST)
    first = turn("cl,xfrl->xfcr", pick, wavefield[..., :LANES]) * mask
    last = turn("cl,xfrl->xfcr", jnp.roll(pick, -SHALF, 1), wavefield[..., shots - LANES :]) * mask
    after = shifted(first, "src", -1)
    before = shifted(last, "src", 1)
    sides = jnp.concatenate([after, before], axis=2)
    sides = jnp.concatenate(
        [
            shifted(sides[..., receivers - HALO :], "rcv", 1),
            sides,
            shifted(sides[..., :HALO], "rcv", -1),
        ],
        axis=3,
    )
    place = jnp.concatenate([pick, jnp.roll(pick, -SHALF, 1)], axis=0)
    side = turn("xfcr,cl->xfrl", sides, place)
    column = mask[:, None]
    mult = None
    energies = []
    for c in range(CHUNKS):
        mult, energy = predict(
            c * size, size, wavefield, column, *halos[c], side, surface_band, band_shift, shot_taper, mult
        )
        energies.append(energy)
    axes = (("src", lax.axis_size("src")), ("rcv", lax.axis_size("rcv")))
    gain = gains(energies, axes, 1)
    prim = subtract(0, slices, gain, wavefield, mult, None)
    return (mult, prim)


def solution(mesh):
    in_specs = (P(None, None, "rcv", "src"), P(None, "rcv", None), P("rcv"), P("rcv"), P())
    out_specs = (P(None, None, "rcv", "src"), P(None, None, "rcv", "src"))
    return jax.shard_map(
        per_device, mesh=mesh, in_specs=in_specs, out_specs=out_specs, check_vma=False
    )
```
